32 devices in a mesh: tm: 4 (over x, core), row: 8 (over z, y).
Axes of the slice: x: 2, y: 2, z: 4, core: 2. Of those that a mesh axis runs over, the one named last changes fastest.
Arguments:
- event_counts: int32 [4, 4096, 4096], P('tm', 'row'), may hold values from 0 to 8
- latent_mean: float32 [4, 4096, 4096], P('tm', 'row'), may hold values from -3 to 3
- latent_var: float32 [4, 4096, 4096], P('tm', 'row'), may hold values from 0.05 to 0.6
- eigen_basis: bfloat16 [4096, 4096], P('row', 'tm'), may hold values from -0.09375 to 0.09375
- spectrum: float32 [4096], replicated, may hold values from 0.2 to 2
- correlation: float32 [1], replicated, may hold values from 0.3 to 0.9
- whitened: float32 [4, 8, 128, 4, 4096], P(None, 'row', None, None, 'tm'), may hold values from -6 to 6
Outputs:
- gradient: float32 [4, 8, 128, 4, 4096], P(None, 'row', None, None, 'tm')
The draws below stay inside these ranges and needn't reach their ends.
All inputs are finite; a program needn't handle non-finite values.
Results may differ from the reference program's by a relative error of at most 0.0045.
Values may be sent and summed in bfloat16 or wider, within the bound.
A program may use at most 128 MiB of HBM per device.

```python
import math
import jax
import jax.numpy as jnp
from jax import lax

N = 4096
TS = 4
QB = 128
N_TM = 4
N_ROW = 8


def set_ends(values, rng, smallest, top_value):
    index_at = [jax.random.randint(jax.random.fold_in(rng, axis), (), 0, length) for axis, length in enumerate(values.shape)]
    longest = values.shape.index(max(values.shape))
    next_to = index_at[:longest] + [(index_at[longest] + 1) % values.shape[longest]] + index_at[longest + 1:]
    return values.at[tuple(index_at)].set(smallest).at[tuple(next_to)].set(top_value)


def shard_levels(rng, extent, split, least, largest):
    def one(dim, shards_of):
        draws = jax.random.uniform(jax.random.fold_in(jax.random.fold_in(rng, 6), dim), (shards_of,), jnp.float32, least / len(split), largest / len(split))
        return jnp.repeat(jnp.exp(draws), extent[dim] // shards_of).reshape((-1,) + (1,) * (len(extent) - dim - 1))

    level = one(*split[0])
    for cut in split[1:]:
        level = level * one(*cut)
    return level


def bell_draw(stream_key, dims, width, reach, shards=(), kind=jnp.bfloat16):
    factor_of = shard_levels(stream_key, dims, shards, -0.22, 0.18) if shards else 1.0
    array = jax.random.normal(stream_key, dims, jnp.float32) * width * factor_of
    return jnp.minimum(jnp.maximum(array, -reach), reach).astype(kind)


def setup_inputs(seed: int = 0) -> dict:
    key_list = jax.random.split(jax.random.key(seed), 8)
    event_counts = set_ends(jax.random.randint(key_list[0], (TS, N, N), 0, 9), jax.random.fold_in(key_list[0], 1), 0, 8).astype(jnp.int32)
    latent_mean = bell_draw(key_list[1], (TS, N, N), 0.7, 3.0, ((0, 4), (1, 8)), jnp.float32)
    latent_var = jnp.clip(jnp.exp(math.log(0.6) - 2.4849067 * jax.random.uniform(key_list[2], (TS, N, N), jnp.float32) ** shard_levels(key_list[2], (TS, N, N), ((0, 4), (1, 8)), -0.2, 0.2)), 0.05, 0.6)
    eigen_basis = bell_draw(key_list[3], (N, N), N ** -0.5, 0.09375, ((0, 8), (1, 4)))
    spectrum = jnp.clip(jnp.exp(jax.random.uniform(key_list[4], (N,), jnp.float32, math.log(0.2), math.log(2.0))), 0.2, 2.0)
    correlation = jnp.clip(jax.random.uniform(key_list[5], (1,), jnp.float32, 0.3, 0.9), 0.3, 0.9)
    whitened = bell_draw(key_list[6], (N_TM, N_ROW, QB, TS, N), 1.0, 6.0, ((1, 8), (4, 4)), jnp.float32)
    return dict(event_counts=event_counts, latent_mean=latent_mean, latent_var=latent_var, eigen_basis=eigen_basis, spectrum=spectrum, correlation=correlation, whitened=whitened)


HERMITE_NODES = (-2.0201828704560856, -0.9585724646138185, 0.0, 0.9585724646138185, 2.0201828704560856)
HERMITE_WEIGHTS = (0.019953242059045913, 0.3936193231522412, 0.9453087204829419, 0.3936193231522412, 0.019953242059045913)

def moments(event_counts, latent_mean, latent_var):
    spread = jnp.sqrt(2.0 * latent_var)
    normal = 1.0 / math.sqrt(math.pi)
    points = [latent_mean + spread * abscissa for abscissa in HERMITE_NODES]
    rate_points = [jnp.exp(value) for value in points]
    mean_rate = sum((weight * normal * value for weight, value in zip(HERMITE_WEIGHTS, rate_points)))
    covariance = sum((weight * normal * (node_value - latent_mean) * (value - mean_rate) for weight, node_value, value in zip(HERMITE_WEIGHTS, points, rate_points)))
    rate_var = sum((weight * normal * (value - mean_rate) * (value - mean_rate) for weight, value in zip(HERMITE_WEIGHTS, rate_points)))
    slope_gain = covariance / latent_var
    noise_var = rate_var - slope_gain * covariance + mean_rate
    return slope_gain * (event_counts.astype(latent_mean.dtype) - mean_rate) / noise_var

def time_factor(correlation, total):
    later = jnp.arange(total)[:, None]
    earlier = jnp.arange(total)[None, :]
    distance = jnp.maximum(later - earlier, 0).astype(correlation.dtype)
    lower = jnp.where(later >= earlier, jnp.power(correlation, distance), jnp.zeros_like(distance))
    column_scale = jnp.where(earlier == 0, jnp.ones_like(distance), jnp.sqrt(1.0 - correlation * correlation) * jnp.ones_like(distance))
    return lower * column_scale

def reference(event_counts, latent_mean, latent_var, eigen_basis, spectrum, correlation, whitened):
    pseudo = moments(event_counts, latent_mean, latent_var).astype(jnp.bfloat16)
    factor = time_factor(correlation[0], TS)
    flat = pseudo.reshape(TS, N * N).astype(factor.dtype)
    mixed_field = jnp.dot(factor.T, flat, precision=lax.Precision.HIGHEST).reshape(TS, N, N).astype(jnp.bfloat16)

    def transform(field):
        partial_y = jnp.dot(field, eigen_basis, preferred_element_type=jnp.float32).astype(jnp.bfloat16)
        return jnp.dot(partial_y.T, eigen_basis, preferred_element_type=jnp.float32)
    mode_values = lax.map(transform, mixed_field)
    root_scale = jnp.sqrt(spectrum)
    scaled = root_scale[None, :, None] * root_scale[None, None, :] * mode_values
    gradient = jnp.transpose(scaled, (1, 0, 2)) - whitened.reshape(N, TS, N)
    return gradient.reshape(N_TM, N_ROW, QB, TS, N)
```

```python
import math

import jax
import jax.numpy as jnp
from jax import lax
from jax.experimental import pallas as pl
from jax.experimental.pallas import tpu as pltpu
from jax.sharding import PartitionSpec as P

HERMITE_NODES = (
    -2.0201828704560856,
    -0.9585724646138185,
    0.0,
    0.9585724646138185,
    2.0201828704560856,
)
HERMITE_WEIGHTS = (
    0.019953242059045913,
    0.3936193231522412,
    0.9453087204829419,
    0.3936193231522412,
    0.019953242059045913,
)


def moments(event_counts, latent_mean, latent_var):
    spread = jnp.sqrt(2.0 * latent_var)
    normal = 1.0 / math.sqrt(math.pi)
    points = [latent_mean + spread * abscissa for abscissa in HERMITE_NODES]
    rate_points = [jnp.exp(value) for value in points]
    mean_rate = sum(
        (weight * normal * value for weight, value in zip(HERMITE_WEIGHTS, rate_points))
    )
    covariance = sum(
        (
            weight * normal * (node_value - latent_mean) * (value - mean_rate)
            for weight, node_value, value in zip(HERMITE_WEIGHTS, points, rate_points)
        )
    )
    rate_var = sum(
        (
            weight * normal * (value - mean_rate) * (value - mean_rate)
            for weight, value in zip(HERMITE_WEIGHTS, rate_points)
        )
    )
    slope_gain = covariance / latent_var
    noise_var = rate_var - slope_gain * covariance + mean_rate
    return slope_gain * (event_counts.astype(latent_mean.dtype) - mean_rate) / noise_var


def time_factor(correlation, total):
    later = jnp.arange(total)[:, None]
    earlier = jnp.arange(total)[None, :]
    distance = jnp.maximum(later - earlier, 0).astype(correlation.dtype)
    lower = jnp.where(later >= earlier, jnp.power(correlation, distance), jnp.zeros_like(distance))
    column_scale = jnp.where(
        earlier == 0,
        jnp.ones_like(distance),
        jnp.sqrt(1.0 - correlation * correlation) * jnp.ones_like(distance),
    )
    return lower * column_scale


VMEM_BYTES = 60 * 1024 * 1024
ROW_CHUNKS = 2
Q_CHUNKS = 2


def exchange(own, axis):
    count = lax.axis_size(axis)
    blocks = [(0, own)]
    bit = count // 2
    while bit:
        pairs = [(i, i ^ bit) for i in range(count)]
        blocks += [(off ^ bit, lax.ppermute(b, axis, pairs)) for off, b in blocks]
        bit //= 2
    return blocks


def first_transform(parts, weights, basis, block_modes, q_chunks):
    row_chunks, total = len(parts), len(parts[0])
    rows, width = parts[0][0].shape
    modes = basis.shape[1]
    tile = min(max(256, block_modes), modes)
    blocks = tile // block_modes
    sub = block_modes // q_chunks

    def kernel(weights_ref, *refs):
        part_refs = refs[: row_chunks * total]
        basis_ref = refs[row_chunks * total]
        out_refs = refs[row_chunks * total + 1 :]
        for c in range(row_chunks):
            fields = [
                jnp.dot(part_refs[c * total + t][...], basis_ref[...], preferred_element_type=jnp.float32)
                for t in range(total)
            ]
            for a in range(total):
                mixed = sum(weights_ref[t, a] * fields[t] for t in range(total))
                turned = mixed.T.astype(jnp.bfloat16).reshape(blocks, block_modes, rows)
                for h in range(q_chunks):
                    out_refs[h][:, a, :, pl.ds(c * rows, rows)] = turned[:, h * sub : (h + 1) * sub, :]

    flat = [p for chunk in parts for p in chunk]
    out = jax.ShapeDtypeStruct((modes // block_modes, total, sub, row_chunks * rows), jnp.bfloat16)
    return pl.pallas_call(
        kernel,
        grid=(modes // tile,),
        in_specs=[pl.BlockSpec(memory_space=pltpu.SMEM)]
        + [pl.BlockSpec((rows, width), lambda i: (0, 0), pipeline_mode=pl.Buffered(1)) for _ in flat]
        + [pl.BlockSpec((width, tile), lambda i: (0, i))],
        out_specs=[pl.BlockSpec((blocks, total, sub, row_chunks * rows), lambda i: (i, 0, 0, 0))] * q_chunks,
        out_shape=[out] * q_chunks,
        compiler_params=pltpu.CompilerParams(vmem_limit_bytes=VMEM_BYTES),
        cost_estimate=pl.CostEstimate(
            flops=2 * total * row_chunks * rows * width * modes,
            bytes_accessed=2 * (total * row_chunks * rows * (width + modes) + width * modes),
            transcendentals=0,
        ),
        name="first_transform",
    )(weights, *flat, basis)


def second_transform(groups, units, basis, scale_y, scale_x, whitened, previous, h, q_chunks):
    count = len(groups)
    sources, total, sub, depth = groups[0].shape
    units_total, _, block_modes, _, band = whitened.shape
    tile = min(256, band)
    width = basis.shape[0]

    def kernel(units_ref, *refs):
        group_refs = refs[:count]
        basis_ref, y_ref, x_ref, whitened_ref = refs[count : count + 4]
        out_ref = refs[-1]
        for s in range(count):
            left = jnp.concatenate(
                [group_refs[s][r].reshape(total * sub, depth) for r in range(sources)], axis=1
            )
            values = jnp.dot(left, basis_ref[...], preferred_element_type=jnp.float32)
            u = units_ref[s]
            scale = y_ref[u] * x_ref[...]
            for a in range(total):
                out_ref[u, 0, :, a, :] = scale * values[a * sub : (a + 1) * sub] - whitened_ref[u, 0, :, a, :]

    field = pl.BlockSpec((units_total, 1, sub, total, tile), lambda i: (0, 0, h, 0, i))
    operands = [units, *groups, basis, scale_y, scale_x, whitened]
    in_specs = (
        [pl.BlockSpec(memory_space=pltpu.SMEM)]
        + [pl.BlockSpec(g.shape, lambda i: (0, 0, 0, 0), pipeline_mode=pl.Buffered(1)) for g in groups]
        + [
            pl.BlockSpec((width, tile), lambda i: (0, i)),
            pl.BlockSpec((units_total, sub, 1), lambda i: (0, h, 0)),
            pl.BlockSpec((1, tile), lambda i: (0, i)),
            field,
        ]
    )
    aliases = {}
    if previous is not None:
        aliases = {len(operands): 0}
        operands.append(previous)
        in_specs.append(pl.BlockSpec(memory_space=pl.ANY))
    return pl.pallas_call(
        kernel,
        grid=(band // tile,),
        in_specs=in_specs,
        out_specs=field,
        out_shape=jax.ShapeDtypeStruct(whitened.shape, jnp.float32),
        input_output_aliases=aliases,
        compiler_params=pltpu.CompilerParams(vmem_limit_bytes=VMEM_BYTES),
        cost_estimate=pl.CostEstimate(
            flops=2 * count * total * sub * width * band,
            bytes_accessed=2 * width * (band + count * total * sub) + 8 * count * total * sub * band,
            transcendentals=0,
        ),
        name="second_transform",
    )(*operands)


def local(event_counts, latent_mean, latent_var, eigen_basis, spectrum, correlation, whitened):
    time_count = lax.axis_size("tm")
    row_devices = lax.axis_size("row")
    here = lax.axis_index("tm")
    total = whitened.shape[3]
    block_modes = whitened.shape[2]
    band_width = eigen_basis.shape[1]
    basis = lax.all_gather(eigen_basis, "row", axis=0, tiled=True)
    rows = event_counts.shape[1]
    row_chunks = ROW_CHUNKS if rows // ROW_CHUNKS % 128 == 0 else 1
    q_chunks = Q_CHUNKS if block_modes // Q_CHUNKS % 16 == 0 else 1
    step = rows // row_chunks
    parts = []
    for c in range(row_chunks):
        cut = [x[0, c * step : (c + 1) * step] for x in (event_counts, latent_mean, latent_var)]
        blocks = exchange(moments(*cut).astype(jnp.bfloat16), "tm")
        parts.append([b for _, b in blocks])
    offsets = jnp.array([off for off, _ in blocks], jnp.int32)
    units = jnp.bitwise_xor(here.astype(jnp.int32), offsets)
    weights = jnp.take(time_factor(correlation[0], total), units, axis=0)
    halves = first_transform(parts, weights, basis, block_modes, q_chunks)
    scale_x = jnp.sqrt(lax.dynamic_slice_in_dim(spectrum, here * band_width, band_width, 0))[None, :]
    scale_y = jnp.sqrt(
        lax.dynamic_slice_in_dim(
            spectrum.reshape(time_count, row_devices, block_modes), lax.axis_index("row"), 1, 1
        ).reshape(time_count, block_modes, 1)
    )
    arrived = [
        [b for _, b in exchange(lax.all_to_all(half, "row", split_axis=0, concat_axis=0, tiled=True), "tm")]
        for half in halves
    ]
    gradient = None
    for h, groups in enumerate(arrived):
        gradient = second_transform(
            groups, units, basis, scale_y, scale_x, whitened, gradient, h, q_chunks
        )
    return gradient


def solution(mesh):
    return jax.shard_map(
        local,
        mesh=mesh,
        in_specs=(
            P("tm", "row", None),
            P("tm", "row", None),
            P("tm", "row", None),
            P("row", "tm"),
            P(),
            P(),
            P(None, "row", None, None, "tm"),
        ),
        out_specs=P(None, "row", None, None, "tm"),
        check_vma=False,
    )
```

```python
import math

import jax
import jax.numpy as jnp
from jax import lax
from jax.experimental import pallas as pl
from jax.experimental.pallas import tpu as pltpu
from jax.sharding import PartitionSpec as P

HERMITE_NODES = (
    -2.0201828704560856,
    -0.9585724646138185,
    0.0,
    0.9585724646138185,
    2.0201828704560856,
)
HERMITE_WEIGHTS = (
    0.019953242059045913,
    0.3936193231522412,
    0.9453087204829419,
    0.3936193231522412,
    0.019953242059045913,
)


def moments(event_counts, latent_mean, latent_var):
    spread = jnp.sqrt(2.0 * latent_var)
    normal = 1.0 / math.sqrt(math.pi)
    points = [latent_mean + spread * abscissa for abscissa in HERMITE_NODES]
    rate_points = [jnp.exp(value) for value in points]
    mean_rate = sum(
        (weight * normal * value for weight, value in zip(HERMITE_WEIGHTS, rate_points))
    )
    covariance = sum(
        (
            weight * normal * (node_value - latent_mean) * (value - mean_rate)
            for weight, node_value, value in zip(HERMITE_WEIGHTS, points, rate_points)
        )
    )
    rate_var = sum(
        (
            weight * normal * (value - mean_rate) * (value - mean_rate)
            for weight, value in zip(HERMITE_WEIGHTS, rate_points)
        )
    )
    slope_gain = covariance / latent_var
    noise_var = rate_var - slope_gain * covariance + mean_rate
    return slope_gain * (event_counts.astype(latent_mean.dtype) - mean_rate) / noise_var


def time_factor(correlation, total):
    later = jnp.arange(total)[:, None]
    earlier = jnp.arange(total)[None, :]
    distance = jnp.maximum(later - earlier, 0).astype(correlation.dtype)
    lower = jnp.where(later >= earlier, jnp.power(correlation, distance), jnp.zeros_like(distance))
    column_scale = jnp.where(
        earlier == 0,
        jnp.ones_like(distance),
        jnp.sqrt(1.0 - correlation * correlation) * jnp.ones_like(distance),
    )
    return lower * column_scale


VMEM_BYTES = 60 * 1024 * 1024
ROW_CHUNKS = 2
Q_CHUNKS = 4


def after(block, value):
    return block + (value * 0.0).astype(block.dtype)


def exchange_step(blocks, axis, bit):
    pairs = [(i, i ^ bit) for i in range(lax.axis_size(axis))]
    return blocks + [(off ^ bit, lax.ppermute(b, axis, pairs)) for off, b in blocks]


def exchange_far(own, axis):
    half = lax.axis_size(axis) // 2
    return exchange_step([(0, own)], axis, half) if half else [(0, own)]


def exchange_near(blocks, axis):
    bit = lax.axis_size(axis) // 4
    while bit:
        blocks = exchange_step(blocks, axis, bit)
        bit //= 2
    return blocks


def first_transform(parts, weights, basis, block_modes, q_chunks):
    row_chunks, total = len(parts), len(parts[0])
    rows, width = parts[0][0].shape
    modes = basis.shape[1]
    tile = min(max(256, block_modes), modes)
    blocks = tile // block_modes
    sub = block_modes // q_chunks

    def kernel(weights_ref, *refs):
        part_refs = refs[: row_chunks * total]
        basis_ref = refs[row_chunks * total]
        out_refs = refs[row_chunks * total + 1 :]
        for c in range(row_chunks):
            fields = [
                jnp.dot(part_refs[c * total + t][...], basis_ref[...], preferred_element_type=jnp.float32)
                for t in range(total)
            ]
            for a in range(total):
                mixed = sum(weights_ref[t, a] * fields[t] for t in range(total))
                turned = mixed.T.astype(jnp.bfloat16).reshape(blocks, block_modes, rows)
                for h in range(q_chunks):
                    out_refs[h][:, a, :, pl.ds(c * rows, rows)] = turned[:, h * sub : (h + 1) * sub, :]

    flat = [p for chunk in parts for p in chunk]
    out = jax.ShapeDtypeStruct((modes // block_modes, total, sub, row_chunks * rows), jnp.bfloat16)
    return pl.pallas_call(
        kernel,
        grid=(modes // tile,),
        in_specs=[pl.BlockSpec(memory_space=pltpu.SMEM)]
        + [pl.BlockSpec((rows, width), lambda i: (0, 0), pipeline_mode=pl.Buffered(1)) for _ in flat]
        + [pl.BlockSpec((width, tile), lambda i: (0, i))],
        out_specs=[pl.BlockSpec((blocks, total, sub, row_chunks * rows), lambda i: (i, 0, 0, 0))] * q_chunks,
        out_shape=[out] * q_chunks,
        compiler_params=pltpu.CompilerParams(vmem_limit_bytes=VMEM_BYTES),
        cost_estimate=pl.CostEstimate(
            flops=2 * total * row_chunks * rows * width * modes,
            bytes_accessed=2 * (total * row_chunks * rows * (width + modes) + width * modes),
            transcendentals=0,
        ),
        name="first_transform",
    )(weights, *flat, basis)


def second_transform(groups, units, basis, scale_y, scale_x, whitened, previous, h, q_chunks):
    count = len(groups)
    sources, total, sub, depth = groups[0].shape
    units_total, _, block_modes, _, band = whitened.shape
    tile = min(256, band)
    width = basis.shape[0]

    def kernel(units_ref, *refs):
        group_refs = refs[:count]
        basis_ref, y_ref, x_ref, whitened_ref = refs[count : count + 4]
        out_ref, done_ref = refs[-2:]
        done_ref[...] = jnp.zeros_like(done_ref)
        for s in range(count):
            left = jnp.concatenate(
                [group_refs[s][r].reshape(total * sub, depth) for r in range(sources)], axis=1
            )
            values = jnp.dot(left, basis_ref[...], preferred_element_type=jnp.float32)
            u = units_ref[s]
            scale = y_ref[u] * x_ref[...]
            for a in range(total):
                out_ref[u, 0, :, a, :] = scale * values[a * sub : (a + 1) * sub] - whitened_ref[u, 0, :, a, :]

    field = pl.BlockSpec((units_total, 1, sub, total, tile), lambda i: (0, 0, h, 0, i))
    operands = [units, *groups, basis, scale_y, scale_x, whitened]
    in_specs = (
        [pl.BlockSpec(memory_space=pltpu.SMEM)]
        + [pl.BlockSpec(g.shape, lambda i: (0, 0, 0, 0), pipeline_mode=pl.Buffered(1)) for g in groups]
        + [
            pl.BlockSpec((width, tile), lambda i: (0, i)),
            pl.BlockSpec((units_total, sub, 1), lambda i: (0, h, 0)),
            pl.BlockSpec((1, tile), lambda i: (0, i)),
            field,
        ]
    )
    aliases = {}
    if previous is not None:
        aliases = {len(operands): 0}
        operands.append(previous)
        in_specs.append(pl.BlockSpec(memory_space=pl.ANY))
    return pl.pallas_call(
        kernel,
        grid=(band // tile,),
        in_specs=in_specs,
        out_specs=[field, pl.BlockSpec((8, 128), lambda i: (0, 0))],
        out_shape=[
            jax.ShapeDtypeStruct(whitened.shape, jnp.float32),
            jax.ShapeDtypeStruct((8, 128), jnp.float32),
        ],
        input_output_aliases=aliases,
        compiler_params=pltpu.CompilerParams(vmem_limit_bytes=VMEM_BYTES),
        cost_estimate=pl.CostEstimate(
            flops=2 * count * total * sub * width * band,
            bytes_accessed=2 * width * (band + count * total * sub) + 8 * count * total * sub * band,
            transcendentals=0,
        ),
        name="second_transform",
    )(*operands)


def local(event_counts, latent_mean, latent_var, eigen_basis, spectrum, correlation, whitened):
    time_count = lax.axis_size("tm")
    row_devices = lax.axis_size("row")
    here = lax.axis_index("tm")
    total = whitened.shape[3]
    block_modes = whitened.shape[2]
    band_width = eigen_basis.shape[1]
    basis = lax.all_gather(eigen_basis, "row", axis=0, tiled=True)
    rows = event_counts.shape[1]
    row_chunks = ROW_CHUNKS if rows // ROW_CHUNKS % 128 == 0 else 1
    q_chunks = Q_CHUNKS if block_modes // Q_CHUNKS % 16 == 0 else 1
    step = rows // row_chunks
    parts = []
    for c in range(row_chunks):
        cut = [x[0, c * step : (c + 1) * step] for x in (event_counts, latent_mean, latent_var)]
        blocks = exchange_near(exchange_far(moments(*cut).astype(jnp.bfloat16), "tm"), "tm")
        parts.append([b for _, b in blocks])
    offsets = jnp.array([off for off, _ in blocks], jnp.int32)
    units = jnp.bitwise_xor(here.astype(jnp.int32), offsets)
    weights = jnp.take(time_factor(correlation[0], total), units, axis=0)
    halves = first_transform(parts, weights, basis, block_modes, q_chunks)
    scale_x = jnp.sqrt(lax.dynamic_slice_in_dim(spectrum, here * band_width, band_width, 0))[None, :]
    scale_y = jnp.sqrt(
        lax.dynamic_slice_in_dim(
            spectrum.reshape(time_count, row_devices, block_modes), lax.axis_index("row"), 1, 1
        ).reshape(time_count, block_modes, 1)
    )
    spread = []
    for h, half in enumerate(halves):
        if h >= 2:
            half = after(half, spread[h - 2][-1][1][0, 0, 0, 0])
        landed = lax.all_to_all(half, "row", split_axis=0, concat_axis=0, tiled=True)
        spread.append(exchange_far(landed, "tm"))
    gradient, done = None, None
    for h, blocks in enumerate(spread):
        if h == q_chunks - 1 and done is not None:
            blocks = blocks[:-1] + [(blocks[-1][0], after(blocks[-1][1], done[0, 0]))]
        groups = [b for _, b in exchange_near(blocks, "tm")]
        gradient, done = second_transform(
            groups, units, basis, scale_y, scale_x, whitened, gradient, h, q_chunks
        )
    return gradient


def solution(mesh):
    return jax.shard_map(
        local,
        mesh=mesh,
        in_specs=(
            P("tm", "row", None),
            P("tm", "row", None),
            P("tm", "row", None),
            P("row", "tm"),
            P(),
            P(),
            P(None, "row", None, None, "tm"),
        ),
        out_specs=P(None, "row", None, None, "tm"),
        check_vma=False,
    )
```
